32 devices in a mesh: dp: 4 (over x, core), expert: 8 (over z, y).
Axes of the slice: x: 2, y: 2, z: 4, core: 2. Of those that a mesh axis runs over, the one named last changes fastest.
Arguments:
- tokens: bfloat16 [128, 256, 1280], P(('dp', 'expert')), may hold values from -32 to 32
- slot_keys: bfloat16 [1280, 8], replicated, may hold values from -20 to 20
- logit_scale: float32 [1], replicated, may hold values from 8 to 16
- up_weight: bfloat16 [8, 1280, 5120], P('expert', None, 'dp'), may hold values from -0.15625 to 0.15625
- up_bias: bfloat16 [8, 5120], P('expert', 'dp'), may hold values from -3 to 3
- down_weight: bfloat16 [8, 5120, 1280], P('expert', 'dp'), may hold values from -0.078125 to 0.078125
- down_bias: bfloat16 [8, 1280], replicated, may hold values from -3 to 3
Outputs:
- mixed_out: bfloat16 [128, 256, 1280], P(('dp', 'expert'))
The draws below stay inside these ranges and needn't reach their ends.
All inputs are finite; a program needn't handle non-finite values.
Results may differ from the reference program's by a relative error of at most 0.017.
Values may be sent and summed in bfloat16 or wider, within the bound.
No kernel may reach another device: no remote copies, remote signals or barrier semaphores. Data moves between devices by JAX's collectives and lax.ppermute only.
A program may use at most 64 MiB of HBM per device.

```python
import math
import jax
import jax.numpy as jnp
from jax import lax

D = 1280
FF = 5120
PATCHES = 256
EXPERTS = 8
IMAGES = 128
N_DP = 4


def slot_basis(key):
    raw = jax.random.normal(jax.random.fold_in(key, 11), (D, EXPERTS), jnp.float32)
    return jnp.clip(raw, -4.0, 4.0)


def draw_slot_keys(key, part):
    basis = slot_basis(key)
    column_scale = jnp.exp(jax.random.uniform(jax.random.fold_in(key, 12), (1, EXPERTS), jnp.float32, math.log(0.5), math.log(5.0)))
    return (basis * column_scale).astype(jnp.bfloat16)


def draw_tokens(key, part):
    basis = slot_basis(key)
    rows_total = IMAGES * PATCHES
    coeffs = jnp.clip(jax.random.normal(jax.random.fold_in(key, 13), (rows_total, EXPERTS), jnp.float32), -4.0, 4.0)
    mixture = 0.2 * jnp.dot(coeffs, jnp.transpose(basis))
    noise = jnp.clip(jax.random.normal(jax.random.fold_in(key, 14), (rows_total, D), jnp.float32), -4.0, 4.0)
    row_scale = jnp.exp(jax.random.uniform(jax.random.fold_in(key, 15), (rows_total, 1), jnp.float32, math.log(0.5), math.log(5.0)))
    values = jnp.clip(row_scale * (noise + mixture), -32.0, 32.0)
    return values.reshape(IMAGES, PATCHES, D).astype(jnp.bfloat16)


def level_of(own_key, shape, pieces, smallest, largest):
    factor_of = 1.0
    for dim, blocks in pieces:
        draws = jax.random.uniform(jax.random.fold_in(jax.random.fold_in(own_key, 6), dim), (blocks,), jnp.float32, smallest / len(pieces), largest / len(pieces))
        factor_of = factor_of * jnp.repeat(jnp.exp(draws), shape[dim] // blocks).reshape((-1,) + (1,) * (len(shape) - 1 - dim))
    return factor_of


def bell_draw(key, dims, scale, bound, cuts=(), held_as=jnp.bfloat16):
    entries = scale * jax.random.normal(key, dims, jnp.float32)
    if cuts:
        entries = entries * level_of(key, dims, cuts, -0.22, 0.18)
    return jnp.clip(entries, -bound, bound).astype(held_as)


def setup_inputs(seed: int = 0) -> dict:
    key_list = jax.random.split(jax.random.key(seed), 8)
    tokens = draw_tokens(jax.random.fold_in(key_list[7], 71), 0)
    slot_keys = draw_slot_keys(jax.random.fold_in(key_list[7], 71), 0)
    logit_scale = jnp.clip(jnp.exp(jax.random.uniform(key_list[2], (1,), jnp.float32, math.log(8.0), math.log(16.0))), 8.0, 16.0)
    up_weight = bell_draw(key_list[3], (EXPERTS, D, FF), D ** -0.5, 0.15625, ((0, 8), (2, 4)))
    up_bias = bell_draw(key_list[4], (EXPERTS, FF), 0.5, 3.0, ((0, 8), (1, 4)))
    down_weight = bell_draw(key_list[5], (EXPERTS, FF, D), FF ** -0.5, 0.078125, ((0, 8), (1, 4)))
    down_bias = bell_draw(key_list[6], (EXPERTS, D), 0.5, 3.0)
    return dict(tokens=tokens, slot_keys=slot_keys, logit_scale=logit_scale, up_weight=up_weight, up_bias=up_bias, down_weight=down_weight, down_bias=down_bias)


norm_eps = 1e-06

def unit_rms(values, axis_pos):
    return values * lax.rsqrt(lax.optimization_barrier(jnp.mean(values * values, axis=axis_pos, keepdims=True)) + norm_eps)

def reference(tokens, slot_keys, logit_scale, up_weight, up_bias, down_weight, down_bias):
    normed_tok = unit_rms(tokens.astype(jnp.float32), 2).astype(jnp.bfloat16)
    normed_keys = unit_rms(slot_keys.astype(jnp.float32), 0).astype(jnp.bfloat16)
    raw_scores = jnp.einsum('ipd,dn->inp', normed_tok.astype(jnp.float32), normed_keys.astype(jnp.float32))
    logits = logit_scale[0] * raw_scores / D
    dispatch = jax.nn.softmax(logits, axis=2).astype(jnp.bfloat16)
    combine = jax.nn.softmax(logits, axis=1).astype(jnp.bfloat16)
    slot_inputs = jnp.einsum('inp,ipd->ind', dispatch.astype(jnp.float32), tokens.astype(jnp.float32)).astype(jnp.bfloat16)

    def one_expert(packed):
        slot_rows, weight_in, bias_in, weight_out = packed
        pre = jnp.dot(slot_rows, weight_in, preferred_element_type=jnp.float32) + bias_in.astype(jnp.float32)[None, :]
        hidden = jax.nn.gelu(pre, approximate=False).astype(jnp.bfloat16)
        blocks = FF // N_DP
        hidden_blocks = jnp.transpose(hidden.reshape(IMAGES, N_DP, blocks), (1, 0, 2))
        weight_blocks = weight_out.reshape(N_DP, blocks, D)
        parts = jnp.einsum('gif,gfd->gid', hidden_blocks.astype(jnp.float32), weight_blocks.astype(jnp.float32))
        parts = parts.astype(jnp.bfloat16)
        return lax.optimization_barrier(jnp.sum(parts.astype(jnp.float32), axis=0))
    summed = lax.map(one_expert, (jnp.transpose(slot_inputs, (1, 0, 2)), up_weight, up_bias, down_weight))
    expert_out = (summed + down_bias.astype(jnp.float32)[:, None, :]).astype(jnp.bfloat16)
    mixed_out = jnp.einsum('inp,nid->ipd', combine.astype(jnp.float32), expert_out.astype(jnp.float32))
    return mixed_out.astype(jnp.bfloat16)
```

```python
import jax
import jax.numpy as jnp
from jax import lax
from jax.sharding import PartitionSpec as P

norm_eps = 1e-06


def unit_rms(values, axis_pos):
    return values * lax.rsqrt(jnp.mean(values * values, axis=axis_pos, keepdims=True) + norm_eps)


def body(tokens, slot_keys, logit_scale, up_weight, up_bias, down_weight, down_bias):
    images = tokens.shape[0]
    patches = tokens.shape[1]
    width = tokens.shape[2]
    per_owner = up_weight.shape[0]
    owners = lax.axis_size("expert")
    normed_tok = unit_rms(tokens.astype(jnp.float32), 2).astype(jnp.bfloat16)
    normed_keys = unit_rms(slot_keys.astype(jnp.float32), 0).astype(jnp.bfloat16)
    raw_scores = jnp.einsum(
        "ipd,dn->inp", normed_tok, normed_keys, preferred_element_type=jnp.float32
    )
    logits = logit_scale[0] * raw_scores / width
    dispatch = jax.nn.softmax(logits, axis=2).astype(jnp.bfloat16)
    combine = jax.nn.softmax(logits, axis=1).astype(jnp.bfloat16)
    slot_inputs = jnp.einsum(
        "inp,ipd->ind", dispatch, tokens, preferred_element_type=jnp.float32
    ).astype(jnp.bfloat16)
    replicas = lax.axis_size("dp")
    everyone = ("dp", "expert")
    outgoing = jnp.transpose(slot_inputs.reshape(images, owners, per_owner, width), (1, 0, 2, 3))
    outgoing = jnp.broadcast_to(outgoing[None], (replicas,) + outgoing.shape).reshape(
        replicas * owners, images, per_owner, width
    )
    gathered = lax.all_to_all(outgoing, everyone, split_axis=0, concat_axis=0, tiled=True)
    pre = jnp.einsum(
        "rkd,kdf->rkf",
        gathered.reshape(replicas * owners * images, per_owner, width),
        up_weight,
        preferred_element_type=jnp.float32,
    )
    pre = pre + up_bias.astype(jnp.float32)[None]
    hidden = jax.nn.gelu(pre, approximate=False).astype(jnp.bfloat16)
    partial = jnp.einsum(
        "rkf,kfd->rkd", hidden, down_weight, preferred_element_type=jnp.float32
    ).astype(jnp.bfloat16)
    parts = lax.all_to_all(
        partial.reshape(replicas * owners, images, per_owner, width),
        everyone,
        split_axis=0,
        concat_axis=0,
        tiled=True,
    )
    summed = jnp.sum(
        parts.reshape(replicas, owners, images, per_owner, width).astype(jnp.float32), axis=0
    )
    bias = down_bias.astype(jnp.float32).reshape(owners, 1, per_owner, width)
    returned = (summed + bias).astype(jnp.bfloat16)
    weights = combine.reshape(images, owners, per_owner, patches)
    mixed_out = jnp.einsum("iekp,eikd->ipd", weights, returned, preferred_element_type=jnp.float32)
    return mixed_out.astype(jnp.bfloat16)


def solution(mesh):
    return jax.shard_map(
        body,
        mesh=mesh,
        in_specs=(
            P(("dp", "expert"), None, None),
            P(),
            P(),
            P("expert", None, "dp"),
            P("expert", "dp"),
            P("expert", "dp", None),
            P(),
        ),
        out_specs=P(("dp", "expert"), None, None),
        check_vma=False,
    )
```

```python
import functools

import jax
import jax.numpy as jnp
from jax import lax
from jax.experimental import pallas as pl
from jax.experimental.pallas import tpu as pltpu
from jax.sharding import PartitionSpec as P

norm_eps = 1e-06
f32 = jnp.float32
bf16 = jnp.bfloat16
vmem = pl.BlockSpec(memory_space=pltpu.VMEM)
smem = pl.BlockSpec(memory_space=pltpu.SMEM)
hbm = pl.BlockSpec(memory_space=pl.ANY)


def front_kernel(replicas, scale_ref, keys_ref, tok_hbm, out_ref, comb_ref, tok, rows, sems):
    images, patches, width = tok.shape
    experts = keys_ref.shape[0]
    copies = [
        pltpu.make_async_copy(tok_hbm.at[i], tok.at[i], sems.at[i]) for i in range(images)
    ]
    for c in copies:
        c.start()
    keys = keys_ref[...].astype(f32)
    keys = keys * lax.rsqrt(jnp.mean(keys * keys, axis=1, keepdims=True) + norm_eps)
    keys = keys.astype(bf16)
    ones = jnp.ones((8, width), bf16)
    scale = scale_ref[0] / width
    nt = (((1,), (1,)), ((), ()))
    for i in range(images):
        copies[i].wait()
        x = tok[i]
        scores = lax.dot_general(keys, x, nt, preferred_element_type=f32)
        squares = lax.dot_general(ones, x * x, nt, preferred_element_type=f32)[0:1]
        logits = scores * (scale * lax.rsqrt(squares / width + norm_eps))
        over_tok = jnp.exp(logits - jnp.max(logits, axis=1, keepdims=True))
        dispatch = over_tok / jnp.sum(over_tok, axis=1, keepdims=True)
        over_slot = jnp.exp(logits - jnp.max(logits, axis=0, keepdims=True))
        comb_ref[i] = (over_slot / jnp.sum(over_slot, axis=0, keepdims=True)).astype(bf16)
        rows[:, i, :] = jnp.dot(dispatch.astype(bf16), x, preferred_element_type=f32)
    packed = rows[...].astype(bf16)
    for r in range(replicas):
        out_ref[r * experts : (r + 1) * experts] = packed


def front(replicas, scale, keys_t, tokens):
    images, patches, width = tokens.shape
    experts = keys_t.shape[0]
    return pl.pallas_call(
        functools.partial(front_kernel, replicas),
        in_specs=[smem, vmem, hbm],
        out_specs=[vmem, vmem],
        out_shape=[
            jax.ShapeDtypeStruct((replicas * experts, images, width), bf16),
            jax.ShapeDtypeStruct((images, experts, patches), bf16),
        ],
        scratch_shapes=[
            pltpu.VMEM((images, patches, width), bf16),
            pltpu.VMEM((experts, images, width), f32),
            pltpu.SemaphoreType.DMA((images,)),
        ],
        name="front",
    )(scale, keys_t, tokens)


def expert_kernel(x_ref, up_ref, up_bias_ref, down_ref, out_ref):
    senders, images, width = x_ref.shape
    x = x_ref[...].astype(f32).reshape(senders * images, width).astype(bf16)
    pre = jnp.dot(x, up_ref[0], preferred_element_type=f32)
    pre = pre + up_bias_ref[...].astype(f32)
    hidden = (0.5 * pre * (1.0 + lax.erf(pre * (0.5**0.5)))).astype(bf16)
    part = jnp.dot(hidden, down_ref[0], preferred_element_type=f32)
    out_ref[...] = part.reshape(senders, images, width).astype(bf16)


def expert(x, up, up_bias, down):
    return pl.pallas_call(
        expert_kernel,
        in_specs=[vmem] * 4,
        out_specs=vmem,
        out_shape=jax.ShapeDtypeStruct(x.shape, bf16),
        name="expert",
    )(x, up, up_bias, down)


def back_kernel(parts_ref, bias_ref, comb_ref, out_hbm, rows, out, sems):
    images, patches, width = out.shape
    experts = bias_ref.shape[0]
    replicas = parts_ref.shape[0] // experts
    total = parts_ref[0:experts].astype(f32)
    for r in range(1, replicas):
        total = total + parts_ref[r * experts : (r + 1) * experts].astype(f32)
    rows[...] = total
    bias = bias_ref[...].astype(f32)
    copies = []
    for i in range(images):
        y = (rows[:, i, :] + bias).astype(bf16)
        mixed = lax.dot_general(
            comb_ref[i], y, (((0,), (0,)), ((), ())), preferred_element_type=f32
        )
        out[i] = mixed.astype(bf16)
        copies.append(pltpu.make_async_copy(out.at[i], out_hbm.at[i], sems.at[i]))
        copies[i].start()
    for c in copies:
        c.wait()


def back(parts, bias, comb):
    images, experts, patches = comb.shape
    width = bias.shape[1]
    shape = (images, patches, width)
    return pl.pallas_call(
        back_kernel,
        in_specs=[vmem] * 3,
        out_specs=hbm,
        out_shape=jax.ShapeDtypeStruct(shape, bf16),
        scratch_shapes=[
            pltpu.VMEM((experts, images, width), f32),
            pltpu.VMEM(shape, bf16),
            pltpu.SemaphoreType.DMA((images,)),
        ],
        name="back",
    )(parts, bias, comb)


def body(tokens, slot_keys, logit_scale, up_weight, up_bias, down_weight, down_bias):
    replicas = lax.axis_size("dp")
    everyone = ("dp", "expert")
    outgoing, comb = front(replicas, logit_scale, slot_keys.T, tokens)
    gathered = lax.all_to_all(outgoing, everyone, split_axis=0, concat_axis=0, tiled=True)
    partial = expert(gathered, up_weight, up_bias, down_weight)
    parts = lax.all_to_all(partial, everyone, split_axis=0, concat_axis=0, tiled=True)
    return back(parts, down_bias, comb)


def solution(mesh):
    return jax.shard_map(
        body,
        mesh=mesh,
        in_specs=(
            P(("dp", "expert"), None, None),
            P(),
            P(),
            P("expert", None, "dp"),
            P("expert", "dp"),
            P("expert", "dp", None),
            P(),
        ),
        out_specs=P(("dp", "expert"), None, None),
        check_vma=False,
    )
```

```python
import functools

import jax
import jax.numpy as jnp
from jax import lax
from jax.experimental import pallas as pl
from jax.experimental.pallas import tpu as pltpu
from jax.sharding import PartitionSpec as P

norm_eps = 1e-06
f32 = jnp.float32
bf16 = jnp.bfloat16
vmem = pl.BlockSpec(memory_space=pltpu.VMEM)
smem = pl.BlockSpec(memory_space=pltpu.SMEM)
hbm = pl.BlockSpec(memory_space=pltpu.HBM)


def front_kernel(
    replicas, scale_ref, keys_ref, tok_hbm, down_hbm, out_ref, comb_ref, down_ref, tok, rows, sems
):
    images, patches, width = tok.shape
    experts = keys_ref.shape[0]
    copies = [
        pltpu.make_async_copy(tok_hbm.at[i], tok.at[i], sems.at[i]) for i in range(images)
    ]
    copies.append(pltpu.make_async_copy(down_hbm, down_ref, sems.at[images]))
    for c in copies:
        c.start()
    keys = keys_ref[...].astype(f32)
    keys = keys * lax.rsqrt(jnp.mean(keys * keys, axis=1, keepdims=True) + norm_eps)
    keys = keys.astype(bf16)
    ones = jnp.ones((8, width), bf16)
    scale = scale_ref[0] / width
    nt = (((1,), (1,)), ((), ()))
    for i in range(images):
        copies[i].wait()
        x = tok[i]
        scores = lax.dot_general(keys, x, nt, preferred_element_type=f32)
        squares = lax.dot_general(ones, x * x, nt, preferred_element_type=f32)[0:1]
        logits = scores * (scale * lax.rsqrt(squares / width + norm_eps))
        over_tok = jnp.exp(logits - jnp.max(logits, axis=1, keepdims=True))
        dispatch = over_tok / jnp.sum(over_tok, axis=1, keepdims=True)
        over_slot = jnp.exp(logits - jnp.max(logits, axis=0, keepdims=True))
        comb_ref[i] = (over_slot / jnp.sum(over_slot, axis=0, keepdims=True)).astype(bf16)
        rows[:, i, :] = jnp.dot(dispatch.astype(bf16), x, preferred_element_type=f32)
    packed = rows[...].astype(bf16)
    for r in range(replicas):
        out_ref[r * experts : (r + 1) * experts] = packed
    copies[images].wait()


def front(replicas, scale, keys_t, tokens, down):
    images, patches, width = tokens.shape
    experts = keys_t.shape[0]
    return pl.pallas_call(
        functools.partial(front_kernel, replicas),
        in_specs=[smem, vmem, hbm, hbm],
        out_specs=[vmem, vmem, vmem],
        out_shape=[
            jax.ShapeDtypeStruct((replicas * experts, images, width), bf16),
            jax.ShapeDtypeStruct((images, experts, patches), bf16),
            pltpu.VMEM(down.shape, bf16),
        ],
        scratch_shapes=[
            pltpu.VMEM((images, patches, width), bf16),
            pltpu.VMEM((experts, images, width), f32),
            pltpu.SemaphoreType.DMA((images + 1,)),
        ],
        compiler_params=pltpu.CompilerParams(vmem_limit_bytes=12 << 20),
        cost_estimate=pl.CostEstimate(
            flops=4 * (experts + 8) * tokens.size,
            transcendentals=2 * images * experts * patches,
            bytes_accessed=8 * tokens.size,
        ),
        name="front",
    )(scale, keys_t, tokens, down)


def expert_kernel(x_ref, up_ref, up_bias_ref, down_ref, out_ref):
    senders, images, width = x_ref.shape
    x = x_ref[...].astype(f32).reshape(senders * images, width).astype(bf16)
    pre = jnp.dot(x, up_ref[0], preferred_element_type=f32)
    pre = pre + up_bias_ref[...].astype(f32)
    hidden = (0.5 * pre * (1.0 + lax.erf(pre * (0.5**0.5)))).astype(bf16)
    part = jnp.dot(hidden, down_ref[0], preferred_element_type=f32)
    out_ref[...] = part.reshape(senders, images, width).astype(bf16)


def expert(x, up, up_bias, down):
    return pl.pallas_call(
        expert_kernel,
        in_specs=[vmem] * 4,
        out_specs=vmem,
        out_shape=jax.ShapeDtypeStruct(x.shape, bf16),
        compiler_params=pltpu.CompilerParams(vmem_limit_bytes=16 << 20),
        name="expert",
    )(x, up, up_bias, down)


def back_kernel(parts_ref, bias_ref, comb_ref, out_hbm, rows, out, sems):
    images, patches, width = out.shape
    experts = bias_ref.shape[0]
    replicas = parts_ref.shape[0] // experts
    total = parts_ref[0:experts].astype(f32)
    for r in range(1, replicas):
        total = total + parts_ref[r * experts : (r + 1) * experts].astype(f32)
    rows[...] = total
    bias = bias_ref[...].astype(f32)
    copies = []
    for i in range(images):
        y = (rows[:, i, :] + bias).astype(bf16)
        mixed = lax.dot_general(
            comb_ref[i], y, (((0,), (0,)), ((), ())), preferred_element_type=f32
        )
        out[i] = mixed.astype(bf16)
        copies.append(pltpu.make_async_copy(out.at[i], out_hbm.at[i], sems.at[i]))
        copies[i].start()
    for c in copies:
        c.wait()


def back(parts, bias, comb):
    images, experts, patches = comb.shape
    width = bias.shape[1]
    shape = (images, patches, width)
    return pl.pallas_call(
        back_kernel,
        in_specs=[vmem] * 3,
        out_specs=hbm,
        out_shape=jax.ShapeDtypeStruct(shape, bf16),
        scratch_shapes=[
            pltpu.VMEM((experts, images, width), f32),
            pltpu.VMEM(shape, bf16),
            pltpu.SemaphoreType.DMA((images,)),
        ],
        compiler_params=pltpu.CompilerParams(vmem_limit_bytes=12 << 20),
        name="back",
    )(parts, bias, comb)


def body(tokens, slot_keys, logit_scale, up_weight, up_bias, down_weight, down_bias):
    replicas = lax.axis_size("dp")
    everyone = ("dp", "expert")
    outgoing, comb, down_near = front(
        replicas,
        logit_scale,
        slot_keys.T,
        pltpu.with_memory_space_constraint(tokens, pltpu.HBM),
        pltpu.with_memory_space_constraint(down_weight, pltpu.HBM),
    )
    gathered = lax.all_to_all(outgoing, everyone, split_axis=0, concat_axis=0, tiled=True)
    partial = expert(gathered, up_weight, up_bias, down_near)
    parts = lax.all_to_all(partial, everyone, split_axis=0, concat_axis=0, tiled=True)
    return back(parts, down_bias, comb)


def solution(mesh):
    return jax.shard_map(
        body,
        mesh=mesh,
        in_specs=(
            P(("dp", "expert"), None, None),
            P(),
            P(),
            P("expert", None, "dp"),
            P("expert", "dp"),
            P("expert", "dp", None),
            P(),
        ),
        out_specs=P(("dp", "expert"), None, None),
        check_vma=False,
    )
```

```python
import functools

import jax
import jax.numpy as jnp
from jax import lax
from jax.experimental import pallas as pl
from jax.experimental.pallas import tpu as pltpu
from jax.sharding import PartitionSpec as P

norm_eps = 1e-06
f32 = jnp.float32
bf16 = jnp.bfloat16
vmem = pl.BlockSpec(memory_space=pltpu.VMEM)
smem = pl.BlockSpec(memory_space=pltpu.SMEM)
hbm = pl.BlockSpec(memory_space=pltpu.HBM)


def front_kernel(
    replicas,
    scale_ref,
    keys_hbm,
    tok_hbm,
    down_hbm,
    out_ref,
    comb_ref,
    down_ref,
    keys_ref,
    tok,
    rows,
    sems,
):
    images, patches, width = tok.shape
    experts = keys_ref.shape[0]
    copies = [
        pltpu.make_async_copy(tok_hbm.at[i], tok.at[i], sems.at[i]) for i in range(images)
    ]
    copies.append(pltpu.make_async_copy(down_hbm, down_ref, sems.at[images]))
    small = [
        pltpu.make_async_copy(keys_hbm, keys_ref, sems.at[images + 1]),
    ]
    for c in small + copies:
        c.start()
    for c in small:
        c.wait()
    keys = keys_ref[...].astype(f32)
    keys = keys * lax.rsqrt(jnp.mean(keys * keys, axis=1, keepdims=True) + norm_eps)
    keys = keys.astype(bf16)
    ones = jnp.ones((8, width), bf16)
    scale = scale_ref[0] / width
    nt = (((1,), (1,)), ((), ()))
    for i in range(images):
        copies[i].wait()
        x = tok[i]
        scores = lax.dot_general(keys, x, nt, preferred_element_type=f32)
        squares = lax.dot_general(ones, x * x, nt, preferred_element_type=f32)[0:1]
        logits = scores * (scale * lax.rsqrt(squares / width + norm_eps))
        over_tok = jnp.exp(logits - jnp.max(logits, axis=1, keepdims=True))
        dispatch = over_tok / jnp.sum(over_tok, axis=1, keepdims=True)
        over_slot = jnp.exp(logits - jnp.max(logits, axis=0, keepdims=True))
        comb_ref[i] = (over_slot / jnp.sum(over_slot, axis=0, keepdims=True)).astype(bf16)
        rows[:, i, :] = jnp.dot(dispatch.astype(bf16), x, preferred_element_type=f32)
    packed = rows[...].astype(bf16)
    for r in range(replicas):
        out_ref[r * experts : (r + 1) * experts] = packed
    copies[images].wait()


def front(replicas, scale, keys_t, tokens, down):
    images, patches, width = tokens.shape
    experts = keys_t.shape[0]
    return pl.pallas_call(
        functools.partial(front_kernel, replicas),
        in_specs=[smem, hbm, hbm, hbm],
        out_specs=[vmem, vmem, vmem],
        out_shape=[
            jax.ShapeDtypeStruct((replicas * experts, images, width), bf16),
            jax.ShapeDtypeStruct((images, experts, patches), bf16),
            pltpu.VMEM(down.shape, bf16),
        ],
        scratch_shapes=[
            pltpu.VMEM(keys_t.shape, bf16),
            pltpu.VMEM((images, patches, width), bf16),
            pltpu.VMEM((experts, images, width), f32),
            pltpu.SemaphoreType.DMA((images + 2,)),
        ],
        compiler_params=pltpu.CompilerParams(vmem_limit_bytes=12 << 20),
        cost_estimate=pl.CostEstimate(
            flops=4 * (experts + 8) * tokens.size,
            transcendentals=2 * images * experts * patches,
            bytes_accessed=8 * tokens.size,
        ),
        name="front",
    )(scale, keys_t, tokens, down)


def expert_kernel(x_ref, up_ref, up_bias_ref, down_ref, out_ref):
    senders, images, width = x_ref.shape
    x = x_ref[...].astype(f32).reshape(senders * images, width).astype(bf16)
    pre = jnp.dot(x, up_ref[0], preferred_element_type=f32)
    pre = pre + up_bias_ref[...].astype(f32)
    hidden = (0.5 * pre * (1.0 + lax.erf(pre * (0.5**0.5)))).astype(bf16)
    part = jnp.dot(hidden, down_ref[0], preferred_element_type=f32)
    out_ref[...] = part.reshape(senders, images, width).astype(bf16)


def expert(x, up, up_bias, down):
    return pl.pallas_call(
        expert_kernel,
        in_specs=[vmem] * 4,
        out_specs=vmem,
        out_shape=jax.ShapeDtypeStruct(x.shape, bf16),
        compiler_params=pltpu.CompilerParams(vmem_limit_bytes=16 << 20),
        name="expert",
    )(x, up, up_bias, down)


def back_kernel(parts_ref, bias_ref, comb_ref, out_hbm, rows, out, sems):
    images, patches, width = out.shape
    experts = bias_ref.shape[0]
    replicas = parts_ref.shape[0] // experts
    total = parts_ref[0:experts].astype(f32)
    for r in range(1, replicas):
        total = total + parts_ref[r * experts : (r + 1) * experts].astype(f32)
    rows[...] = total
    bias = bias_ref[...].astype(f32)
    copies = []
    for i in range(images):
        y = (rows[:, i, :] + bias).astype(bf16)
        mixed = lax.dot_general(
            comb_ref[i], y, (((0,), (0,)), ((), ())), preferred_element_type=f32
        )
        out[i] = mixed.astype(bf16)
        copies.append(pltpu.make_async_copy(out.at[i], out_hbm.at[i], sems.at[i]))
        copies[i].start()
    for c in copies:
        c.wait()


def back(parts, bias, comb):
    images, experts, patches = comb.shape
    width = bias.shape[1]
    shape = (images, patches, width)
    return pl.pallas_call(
        back_kernel,
        in_specs=[vmem] * 3,
        out_specs=hbm,
        out_shape=jax.ShapeDtypeStruct(shape, bf16),
        scratch_shapes=[
            pltpu.VMEM((experts, images, width), f32),
            pltpu.VMEM(shape, bf16),
            pltpu.SemaphoreType.DMA((images,)),
        ],
        compiler_params=pltpu.CompilerParams(vmem_limit_bytes=12 << 20),
        name="back",
    )(parts, bias, comb)


def body(tokens, slot_keys, logit_scale, up_weight, up_bias, down_weight, down_bias):
    replicas = lax.axis_size("dp")
    everyone = ("dp", "expert")
    outgoing, comb, down_near = front(
        replicas,
        logit_scale,
        pltpu.with_memory_space_constraint(slot_keys.T, pltpu.HBM),
        pltpu.with_memory_space_constraint(tokens, pltpu.HBM),
        pltpu.with_memory_space_constraint(down_weight, pltpu.HBM),
    )
    gathered = lax.all_to_all(outgoing, everyone, split_axis=0, concat_axis=0, tiled=True)
    partial = expert(gathered, up_weight, up_bias, down_near)
    parts = lax.all_to_all(partial, everyone, split_axis=0, concat_axis=0, tiled=True)
    return back(parts, down_bias, comb)


def solution(mesh):
    return jax.shard_map(
        body,
        mesh=mesh,
        in_specs=(
            P(("dp", "expert"), None, None),
            P(),
            P(),
            P("expert", None, "dp"),
            P("expert", "dp"),
            P("expert", "dp", None),
            P(),
        ),
        out_specs=P(("dp", "expert"), None, None),
        check_vma=False,
    )
```
